32 devices in a mesh: dp: 8 (over y, x, core), tensor: 4 (over z).
Axes of the slice: x: 2, y: 2, z: 4, core: 2. Of those that a mesh axis runs over, the one named last changes fastest.
Arguments:
- attn_out: bfloat16 [8192, 3072], P('dp', 'tensor'), may hold values from -6 to 6
- cotangent: bfloat16 [8192, 2560], P(('dp', 'tensor')), may hold values from -0.1875 to 0.1875
- residual: bfloat16 [8, 3072, 2560], P('dp', 'tensor'), may hold values from -6 to 6
- local_offsets: int32 [8, 4, 8, 48], P('dp', 'tensor'), may hold values from 0 to 2399, as said below
- local_counts: int32 [8, 4, 8], P('dp', 'tensor'), may hold values from 1 to 48, as said below
- kept_offsets: int32 [4, 8, 12], P('tensor'), may hold values from 0 to 2399, as said below
- kept_counts: int32 [4, 8], P('tensor'), may hold values from 6 to 12, as said below
- bounds: int32 [9], replicated, may hold values from 0 to 15360, as said below
Outputs:
- new_residual: bfloat16 [8, 3072, 2560], P('dp', 'tensor')
- kept_sums: float32 [4, 8, 12, 128], P('tensor')
The draws below stay inside these ranges and needn't reach their ends.
Inputs may be any that keep to these rules, and one draw needn't show every extreme that they name: `local_offsets`: for each replica, band and region the 48 entries are different offsets within the region (below bounds[r + 1] - bounds[r]); slots at or past local_counts are ignored but hold such offsets too. `local_counts`: for each band, some region has 48 live slots from every replica. `kept_offsets`: for each band and region the 12 entries are different offsets within the region; slots at or past kept_counts are ignored. `kept_counts`: for each band, some region has 12 live kept slots. bounds[0] = 0, bounds[8] = 15360, rising; each region holds 1440 to 2400 blocks.
All inputs are finite; a program needn't handle non-finite values.
Results may differ from the reference program's by a relative error of at most 0.001.
Values may be sent and summed in bfloat16 or wider, within the bound.
No kernel may reach another device: no remote copies, remote signals or barrier semaphores. Data moves between devices by JAX's collectives and lax.ppermute only.
A program may use at most 64 MiB of HBM per device.

```python
import jax
import jax.numpy as jnp
from jax import lax

D = 2560
HEADS = 24
HD = 128
TOK_REP = 1024
CAP = 48
GCAP = 12
TOKENS = 8192
REGION = 1920
N_DP = 8
N_TENSOR = 4


def region_layout(key):
    pair_count = N_DP // 2
    widening = jax.random.randint(jax.random.fold_in(key, 101), (pair_count,), 0, REGION // 4 + 1)
    widest_pair = jax.random.randint(jax.random.fold_in(key, 107), (), 0, pair_count)
    widening = jnp.where(jnp.arange(pair_count) == widest_pair, REGION // 4, widening)
    region_sizes = jnp.stack([REGION + widening, REGION - widening], axis=1).reshape(-1).astype(jnp.int32)
    region_bounds = jnp.concatenate([jnp.zeros((1,), jnp.int32), jnp.cumsum(region_sizes).astype(jnp.int32)])
    widest = REGION + REGION // 4
    random_keys = jax.random.randint(jax.random.fold_in(key, 102), (N_TENSOR, N_DP, widest), 0, 1 << 16)
    ranked = random_keys * widest + jnp.arange(widest, dtype=jnp.int32)[None, None, :]
    shuffle = jnp.argsort(ranked, axis=-1).astype(jnp.int32)
    outside = (shuffle >= region_sizes[None, :, None]).astype(jnp.int32)
    arranged = jnp.argsort(outside * widest + jnp.arange(widest, dtype=jnp.int32)[None, None, :], axis=-1)
    shuffled = jnp.take_along_axis(shuffle, arranged, axis=-1)
    return (region_bounds, shuffled[:, :, :GCAP + CAP])


def draw_bounds(key, part):
    return region_layout(key)[0]


def draw_local_offsets(key, part):
    region_bounds, shuffled = region_layout(key)
    offset_start = jax.random.randint(jax.random.fold_in(key, 103), (N_DP, N_TENSOR, N_DP, 1), 0, GCAP)
    window_pos = offset_start + jnp.arange(CAP, dtype=jnp.int32)[None, None, None, :]
    spread_lists = jnp.broadcast_to(shuffled[None], (N_DP,) + shuffled.shape)
    return jnp.take_along_axis(spread_lists, window_pos, axis=-1).astype(jnp.int32)


def draw_local_counts(key, part):
    heat_level = jax.random.randint(jax.random.fold_in(key, 104), (N_TENSOR, N_DP), 1, 5)
    ceiling = CAP * heat_level // 4
    floor_count = jnp.maximum(ceiling // 2, 1)
    counts_drawn = jax.random.randint(jax.random.fold_in(key, 105), (N_DP, N_TENSOR, N_DP), floor_count[None], ceiling[None] + 1)
    busiest = jax.random.randint(jax.random.fold_in(key, 106), (N_TENSOR,), 0, N_DP)
    counts_drawn = jnp.where(jnp.arange(N_DP)[None, None, :] == busiest[None, :, None], CAP, counts_drawn)
    return counts_drawn.astype(jnp.int32)


def draw_kept_offsets(key, part):
    region_bounds, shuffled = region_layout(key)
    return shuffled[:, :, :GCAP].astype(jnp.int32)


def draw_kept_counts(key, part):
    counts_drawn = jax.random.randint(jax.random.fold_in(key, 108), (N_TENSOR, N_DP), GCAP // 2, GCAP + 1)
    busiest = jax.random.randint(jax.random.fold_in(key, 109), (N_TENSOR,), 0, N_DP)
    counts_drawn = jnp.where(jnp.arange(N_DP)[None, :] == busiest[:, None], GCAP, counts_drawn)
    return counts_drawn.astype(jnp.int32)


def block_levels(own_key, extent, shards, smallest, largest):
    factor_of, own = 1.0, jax.random.fold_in(own_key, 6)
    for position, parts in shards:
        steps = jnp.exp(jax.random.uniform(jax.random.fold_in(own, position), (parts,), jnp.float32, smallest / len(shards), largest / len(shards)))
        factor_of = factor_of * jnp.repeat(steps, extent[position] // parts).reshape([-1 if axis == position else 1 for axis in range(len(extent))])
    return factor_of


def scatter_about(key, shape, spread, reach, cuts=(), held_as=jnp.bfloat16):
    factor_of = block_levels(key, shape, cuts, -0.22, 0.18) if cuts else 1.0
    values = jax.random.normal(key, shape, jnp.float32) * spread * factor_of
    return jnp.minimum(jnp.maximum(values, -reach), reach).astype(held_as)


def setup_inputs(seed: int = 0) -> dict:
    key_of = jax.random.split(jax.random.key(seed), 9)
    return {
        "attn_out": scatter_about(key_of[0], (TOKENS, HEADS * HD), 1.0, 6.0, ((0, 8), (1, 4))),
        "cotangent": scatter_about(key_of[1], (TOKENS, D), TOK_REP ** -0.5, 0.1875, ((0, 32),)),
        "residual": scatter_about(key_of[2], (N_DP, HEADS * HD, D), 1.0, 6.0, ((0, 8), (1, 4))),
        "local_offsets": draw_local_offsets(jax.random.fold_in(key_of[8], 71), 0),
        "local_counts": draw_local_counts(jax.random.fold_in(key_of[8], 71), 0),
        "kept_offsets": draw_kept_offsets(jax.random.fold_in(key_of[8], 71), 0),
        "kept_counts": draw_kept_counts(jax.random.fold_in(key_of[8], 71), 0),
        "bounds": draw_bounds(jax.random.fold_in(key_of[8], 71), 0),
    }


def pick_rows(block_rows, positions):
    return block_rows[positions]


def mark_sent(positions, live_slots, block_total):
    return jnp.zeros((block_total,), jnp.float32).at[positions.reshape(-1)].max(live_slots.reshape(-1).astype(jnp.float32))


def reference(attn_out, cotangent, residual, local_offsets, local_counts, kept_offsets, kept_counts, bounds):
    attn_rows = attn_out.reshape(N_DP, TOK_REP, HEADS * HD)
    cot_rows = cotangent.reshape(N_DP, TOK_REP, D)
    region_starts = bounds[:N_DP].astype(jnp.int32)

    def replica_step(running, item):
        attn_block, cot_block, res_block, offs_block, counts_block = item
        gradient = lax.dot_general(attn_block, cot_block, (((0,), (0,)), ((), ())), preferred_element_type=jnp.float32)
        accumulated = res_block.astype(jnp.float32) + gradient
        blocks = accumulated.reshape(N_TENSOR, -1, 128)
        block_total = blocks.shape[1]
        live_slots = jnp.arange(CAP)[None, None, :] < counts_block[:, :, None]
        where_abs = (region_starts[None, :, None] + offs_block).astype(jnp.int32)
        picked = jax.vmap(pick_rows)(blocks, where_abs) * live_slots[..., None].astype(jnp.float32)
        sent_mask = jax.vmap(mark_sent, in_axes=(0, 0, None))(where_abs, live_slots, block_total)
        refreshed = (blocks * (1.0 - sent_mask[..., None])).reshape(accumulated.shape).astype(jnp.bfloat16)
        matches = (kept_offsets[:, :, :, None] == offs_block[:, :, None, :]).astype(jnp.float32)
        running = running + jnp.einsum("trji,tric->trjc", matches, picked, precision=lax.Precision.HIGHEST)
        return running, refreshed

    empty_sums = jnp.zeros((N_TENSOR, N_DP, GCAP, 128), jnp.float32)
    summed_all, new_residual = lax.scan(replica_step, empty_sums, (attn_rows, cot_rows, residual, local_offsets, local_counts))
    kept_live = (jnp.arange(GCAP)[None, None, :] < kept_counts[:, :, None]).astype(jnp.float32)
    kept_sums = summed_all * kept_live[..., None]
    return new_residual, kept_sums
```

```python
import functools

import jax
import jax.numpy as jnp
from jax import lax
from jax.experimental import pallas as pl
from jax.experimental.pallas import tpu as pltpu
from jax.sharding import PartitionSpec as P

LANES = 128


def dot(a, b):
    return lax.dot_general(a, b, (((1,), (0,)), ((), ())), preferred_element_type=jnp.float32)


def first_kernel(index_ref, attn_ref, piece_ref, residual_ref, out_ref):
    out_ref[...] = residual_ref[...].astype(jnp.float32) + dot(attn_ref[...], piece_ref[...])


def add_kernel(index_ref, attn_up_ref, attn_down_ref, up_ref, down_ref, acc_ref, out_ref):
    out_ref[...] = acc_ref[...] + (
        dot(attn_up_ref[...], up_ref[...]) + dot(attn_down_ref[...], down_ref[...])
    )


def last_kernel(index_ref, attn_ref, up_ref, down_ref, acc_ref, sent_ref, *rest, first):
    out_ref = rest[-1]
    total = acc_ref[...] + dot(attn_ref[...], up_ref[...] + down_ref[...])
    width = total.shape[1]
    block = pl.program_id(0) * (width // LANES) + first
    spread = (
        lax.broadcasted_iota(jnp.int32, (LANES, width), 0)
        == lax.broadcasted_iota(jnp.int32, (LANES, width), 1) // LANES + block
    ).astype(jnp.bfloat16)
    sent = dot(sent_ref[...], spread)
    out_ref[...] = jnp.where(sent > 0.5, 0.0, total).astype(out_ref.dtype)


def tile_of(width):
    for tile in (512, 384, 256, 128):
        if width % tile == 0:
            return tile
    return width


def first_step(where, attn_t, piece, residual, column):
    rows, tokens = attn_t.shape[0], piece.shape[0]
    width = piece.shape[1]
    tile = tile_of(width)
    base = column // tile
    return pl.pallas_call(
        first_kernel,
        grid_spec=pltpu.PrefetchScalarGridSpec(
            num_scalar_prefetch=1,
            grid=(width // tile,),
            in_specs=[
                pl.BlockSpec((rows, tokens), lambda i, w: (0, w[0])),
                pl.BlockSpec((tokens, tile), lambda i, w: (0, i)),
                pl.BlockSpec((rows, tile), lambda i, w: (0, i + base)),
            ],
            out_specs=pl.BlockSpec((rows, tile), lambda i, w: (0, i)),
        ),
        out_shape=jax.ShapeDtypeStruct((rows, width), jnp.float32),
        cost_estimate=pl.CostEstimate(
            flops=2 * rows * width * tokens, bytes_accessed=6 * rows * width, transcendentals=0
        ),
    )(where, attn_t, piece, residual)


def add_step(where, attn_t, up, down, acc):
    rows, tokens = attn_t.shape[0], up.shape[0]
    width = up.shape[1]
    tile = tile_of(width)
    return pl.pallas_call(
        add_kernel,
        grid_spec=pltpu.PrefetchScalarGridSpec(
            num_scalar_prefetch=1,
            grid=(width // tile,),
            in_specs=[
                pl.BlockSpec((rows, tokens), lambda i, w: (0, w[0])),
                pl.BlockSpec((rows, tokens), lambda i, w: (0, w[1])),
                pl.BlockSpec((tokens, tile), lambda i, w: (0, i)),
                pl.BlockSpec((tokens, tile), lambda i, w: (0, i)),
                pl.BlockSpec((rows, tile), lambda i, w: (0, i)),
            ],
            out_specs=pl.BlockSpec((rows, tile), lambda i, w: (0, i)),
        ),
        out_shape=jax.ShapeDtypeStruct((rows, width), jnp.float32),
        input_output_aliases={5: 0},
        cost_estimate=pl.CostEstimate(
            flops=4 * rows * width * tokens, bytes_accessed=8 * rows * width, transcendentals=0
        ),
    )(where, attn_t, attn_t, up, down, acc)


def last_step(where, attn_t, up, down, acc, sent, column, columns, before):
    rows, tokens = attn_t.shape[0], up.shape[0]
    width = up.shape[1]
    tile = tile_of(width)
    base = column // tile
    in_specs = [
        pl.BlockSpec((rows, tokens), lambda i, w: (0, w[0])),
        pl.BlockSpec((tokens, tile), lambda i, w: (0, i)),
        pl.BlockSpec((tokens, tile), lambda i, w: (0, i)),
        pl.BlockSpec((rows, tile), lambda i, w: (0, i)),
        pl.BlockSpec((rows, LANES), lambda i, w: (0, 0)),
    ]
    operands = [where, attn_t, up, down, acc, sent]
    aliases = {}
    if before is not None:
        in_specs.append(pl.BlockSpec(memory_space=pl.ANY))
        operands.append(before)
        aliases = {len(operands) - 1: 0}
    return pl.pallas_call(
        functools.partial(last_kernel, first=column // LANES),
        grid_spec=pltpu.PrefetchScalarGridSpec(
            num_scalar_prefetch=1,
            grid=(width // tile,),
            in_specs=in_specs,
            out_specs=pl.BlockSpec((rows, tile), lambda i, w: (0, i + base)),
        ),
        out_shape=jax.ShapeDtypeStruct((rows, columns), jnp.bfloat16),
        input_output_aliases=aliases,
        cost_estimate=pl.CostEstimate(
            flops=2 * rows * width * tokens, bytes_accessed=6 * rows * width, transcendentals=0
        ),
    )(*operands)


def on_device(
    ranks,
    attn_out,
    cotangent,
    residual,
    local_offsets,
    local_counts,
    kept_offsets,
    kept_counts,
    bounds,
):
    me = lax.axis_index("tensor")
    tokens, columns = cotangent.shape
    rows = attn_out.shape[1]
    col_blocks = columns // LANES
    cut = (columns // LANES // 2) * LANES
    chunks = [(0, cut), (cut, columns)]

    own = [cotangent[:, a:b] for a, b in chunks]
    ups, downs = [own], [own]
    for step in range(1, ranks):
        ups.append(
            [lax.ppermute(x, "tensor", [(i, i + 1) for i in range(step - 1, ranks - 1)]) for x in ups[-1]]
        )
        downs.append(
            [lax.ppermute(x, "tensor", [(i, i - 1) for i in range(1, ranks - step + 1)]) for x in downs[-1]]
        )

    attn_t = attn_out.T
    res = residual[0]
    regions, slots = local_offsets.shape[2:]
    starts = bounds[:regions]
    offsets, counts = local_offsets[0, 0], local_counts[0, 0]
    live = jnp.arange(slots)[None, :] < counts[:, None]
    where_abs = (starts[:, None] + offsets).reshape(-1)
    row_hot = (
        (where_abs // col_blocks)[:, None] == jnp.arange(rows)[None, :]
    ) & live.reshape(-1)[:, None]
    col_hot = (where_abs % col_blocks)[:, None] == jnp.arange(LANES)[None, :]
    sent = lax.dot_general(
        row_hot.astype(jnp.bfloat16),
        col_hot.astype(jnp.bfloat16),
        (((0,), (0,)), ((), ())),
        preferred_element_type=jnp.float32,
    ).astype(jnp.bfloat16)

    kept, kept_total = kept_offsets[0], kept_counts[0]
    caps = kept.shape[1]
    kept_live = jnp.arange(caps)[None, :] < kept_total[:, None]
    found = jnp.any((kept[:, :, None] == offsets[:, None, :]) & live[:, None, :], axis=2) & kept_live
    kept_abs = (starts[:, None] + kept).reshape(-1)
    kept_row_hot = (
        ((kept_abs // col_blocks)[:, None] == jnp.arange(rows)[None, :]) & found.reshape(-1)[:, None]
    ).astype(jnp.bfloat16)
    kept_col_hot = ((kept_abs % col_blocks)[:, None] == jnp.arange(col_blocks)[None, :]).astype(jnp.float32)
    lists = kept_abs.shape[0]
    kept_attn = lax.dot_general(
        kept_row_hot, attn_out, (((1,), (1,)), ((), ())), preferred_element_type=jnp.float32
    ).astype(jnp.bfloat16)

    def rank_slice(rank):
        return lax.dynamic_slice_in_dim(kept_attn, lax.rem(rank + ranks, ranks) * tokens, tokens, 1)

    picked = []
    accs = []
    for h, (a, b) in enumerate(chunks):
        acc = first_step(me[None], attn_t, own[h], res, a)
        wide = dot(kept_row_hot, res[:, a:b]) + dot(rank_slice(me), own[h])
        for step in range(1, ranks):
            wide = wide + dot(rank_slice(me - step), ups[step][h]) + dot(rank_slice(me + step), downs[step][h])
            if step < ranks - 1:
                where = jnp.stack([lax.rem(me - step + ranks, ranks), lax.rem(me + step, ranks)])
                acc = add_step(where, attn_t, ups[step][h], downs[step][h], acc)
        accs.append(acc)
        hot = kept_col_hot[:, a // LANES : b // LANES]
        picked.append(jnp.sum(wide.reshape(lists, -1, LANES) * hot[:, :, None], axis=1))
    far = jnp.where(me == 0, ranks - 1, 0)[None]
    out = None
    for h, (a, b) in enumerate(chunks):
        out = last_step(far, attn_t, ups[-1][h], downs[-1][h], accs[h], sent, a, columns, out)

    mine = functools.reduce(jnp.add, picked)
    every = lax.all_gather(mine, "dp", axis=0)
    summed = jnp.sum(every, axis=0)
    return (out[None], summed.reshape(1, regions, caps, LANES))


def solution(mesh):
    in_specs = (
        P("dp", "tensor"),
        P(("dp", "tensor"), None),
        P("dp", "tensor", None),
        P("dp", "tensor", None, None),
        P("dp", "tensor", None),
        P("tensor", None, None),
        P("tensor", None),
        P(),
    )
    out_specs = (P("dp", "tensor", None), P("tensor", None, None, None))
    return jax.shard_map(
        functools.partial(on_device, mesh.shape["tensor"]),
        mesh=mesh,
        in_specs=in_specs,
        out_specs=out_specs,
        check_vma=False,
    )
```
